32 devices in a mesh: dp: 8 (over z, x), mp: 4 (over y, core).
Axes of the slice: x: 2, y: 2, z: 4, core: 2. Of those that a mesh axis runs over, the one named last changes fastest.
Arguments:
- acts: bfloat16 [2048, 4096], P('dp'), may hold values from -6 to 6
- cotangent: bfloat16 [2048, 2048], P('dp', 'mp'), may hold values from -0.13183594 to 0.13183594
- stats: float32 [4, 8, 2, 512, 512], P('mp', 'dp'), as said below
- owner_slot: int32 [8], replicated, may hold values from 0 to 7, as said below
Outputs:
- update: bfloat16 [8, 512, 2048], P(None, 'dp', 'mp')
- new_stats: float32 [4, 8, 2, 512, 512], P('mp', 'dp')
The draws below stay inside these ranges and needn't reach their ends.
Inputs may be any that keep to these rules, and one draw needn't show every extreme that they name: Distinct slot numbers; row block w is held by device owner_slot[w] // 1 of dp at its position owner_slot[w] % 1; some device holds 1 block. Every stats[j, s, f] is a symmetric positive definite matrix.
All inputs are finite; a program needn't handle non-finite values.
Results may differ from the reference program's by a relative error of at most 0.012.
The reference program's roundings to bfloat16 on the way (of `gradient`) count: a program that leaves them out, or rounds other values in their place, can miss the bound.
Values may be sent and summed in bfloat16 or wider, within the bound.
A program may use at most 192 MiB of HBM per device.

```python
import jax
import jax.numpy as jnp
from jax import lax

BLK = 512
SLOTS = 1
ITERS = 5
RB = 8
HID = 4096
COLS = 2048
TOKENS = 2048
N_DP = 8
N_MP = 4


def draw_stats(key, part):
    full_shape = (N_MP, N_DP * SLOTS, 2, BLK, BLK)
    key_off, key_diag = jax.random.split(jax.random.fold_in(key, 11), 2)
    off_noise = 0.1 * jax.random.normal(key_off, full_shape, jnp.float32)
    symmetric = 0.5 * (off_noise + jnp.swapaxes(off_noise, -1, -2))
    identity = jnp.eye(BLK, dtype=jnp.float32)
    off_part = symmetric * (1.0 - identity)
    row_weight = jnp.sum(jnp.abs(off_part), axis=-1)
    dominance = jax.random.uniform(key_diag, full_shape[:-1], jnp.float32, 1.05, 2.0)
    matrix = off_part + identity * (row_weight * dominance)[..., None]
    return matrix


def draw_owner_slot(key, part):
    key_devices, key_places, key_order = jax.random.split(jax.random.fold_in(key, 23), 3)
    holders = RB - SLOTS + 1
    devices = jax.random.permutation(key_devices, N_DP)[:holders].astype(jnp.int32)
    places = jax.random.randint(key_places, (holders,), 0, SLOTS).astype(jnp.int32)
    first_owner = devices[0] * SLOTS + jnp.arange(SLOTS, dtype=jnp.int32)
    other_owners = devices[1:] * SLOTS + places[1:]
    slot_list = jnp.concatenate([first_owner, other_owners])
    shuffle = jax.random.permutation(key_order, RB)
    return slot_list[shuffle].astype(jnp.int32)


def block_scale(rng, shape, shards, smallest, largest):
    loudness = 1.0
    for dim, parts in shards:
        draws = jax.random.uniform(jax.random.fold_in(jax.random.fold_in(rng, 6), dim), (parts,), jnp.float32, smallest / len(shards), largest / len(shards))
        loudness = loudness * jnp.repeat(jnp.exp(draws), shape[dim] // parts).reshape((-1,) + (1,) * (len(shape) - 1 - dim))
    return loudness


def centred(own_key, extent, width, bound, cuts=(), kind=jnp.bfloat16):
    level = block_scale(own_key, extent, cuts, -0.22, 0.18) if cuts else 1.0
    values = jax.random.normal(own_key, extent, jnp.float32) * width * level
    return jnp.minimum(jnp.maximum(values, -bound), bound).astype(kind)


def setup_inputs(seed: int = 0) -> dict:
    streams_of = jax.random.split(jax.random.key(seed), 5)
    return {
        "acts": centred(streams_of[0], (TOKENS, HID), 1.0, 6.0, ((0, 8),)),
        "cotangent": centred(streams_of[1], (TOKENS, COLS), (1.0 / TOKENS ** 0.5), 0.13183594, ((0, 8), (1, 4))),
        "stats": draw_stats(jax.random.fold_in(streams_of[4], 71), 0),
        "owner_slot": draw_owner_slot(jax.random.fold_in(streams_of[4], 71), 0),
    }


BETA = 0.9
DAMPING = 0.001
EPSILON = 1e-06

def matmul(former, latter):
    return jnp.dot(former.astype(jnp.bfloat16), latter.astype(jnp.bfloat16), preferred_element_type=jnp.float32)

def inverse_root(statistic):
    identity = jnp.eye(statistic.shape[0], dtype=jnp.float32)
    damped = statistic + DAMPING * identity
    frob_norm = jnp.sqrt(jnp.sum(damped * damped) + EPSILON)
    moment = damped / frob_norm
    result = identity
    for iteration in range(ITERS):
        factor = (5.0 * identity - moment) * 0.25
        if iteration == 0:
            result = factor
        else:
            result = matmul(result, factor)
        if iteration + 1 < ITERS:
            square = matmul(factor, factor)
            moment = matmul(square, matmul(square, moment))
    return result * frob_norm ** (-0.25)

def precondition(grad_block, stat_pair):
    gram_left = jnp.dot(grad_block, grad_block.T, preferred_element_type=jnp.float32)
    gram_right = jnp.dot(grad_block.T, grad_block, preferred_element_type=jnp.float32)
    fresh_left = BETA * stat_pair[0] + (1.0 - BETA) * gram_left
    fresh_right = BETA * stat_pair[1] + (1.0 - BETA) * gram_right
    root_left = inverse_root(fresh_left)
    root_right = inverse_root(fresh_right)
    direction = matmul(matmul(root_left, grad_block), root_right)
    grad_wide = grad_block.astype(jnp.float32)
    graft_ratio = jnp.sqrt((jnp.mean(grad_wide * grad_wide) + EPSILON) / (jnp.mean(direction * direction) + EPSILON))
    return ((direction * graft_ratio).astype(jnp.bfloat16), jnp.stack([fresh_left, fresh_right]))

def reference(acts, cotangent, stats, owner_slot):
    gradient = jnp.dot(acts.T, cotangent, preferred_element_type=jnp.float32).astype(jnp.bfloat16)
    update = jnp.zeros((HID, COLS), jnp.bfloat16)
    zero_index = jnp.zeros((), jnp.int32)

    def one_block(counter, carry):
        stat_store, update_store = carry
        shard = (counter // RB).astype(jnp.int32)
        block_id = (counter % RB).astype(jnp.int32)
        row_start = (block_id * BLK).astype(jnp.int32)
        col_start = (shard * BLK).astype(jnp.int32)
        grad_block = lax.dynamic_slice(gradient, (row_start, col_start), (BLK, BLK))
        slot_id = owner_slot[block_id].astype(jnp.int32)
        stat_pair = lax.dynamic_slice(stat_store, (shard, slot_id, zero_index, zero_index, zero_index), (1, 1, 2, BLK, BLK))[0, 0]
        direction, fresh = precondition(grad_block, stat_pair)
        stat_store = lax.dynamic_update_slice(stat_store, fresh[None, None], (shard, slot_id, zero_index, zero_index, zero_index))
        update_store = lax.dynamic_update_slice(update_store, direction, (row_start, col_start))
        return (stat_store, update_store)
    new_stats, update = lax.fori_loop(0, N_MP * RB, one_block, (stats, update))
    return (update.reshape(RB, BLK, COLS), new_stats)
```

```python
import jax
import jax.numpy as jnp
from jax import lax
from jax.experimental import pallas as pl
from jax.experimental.pallas import tpu as pltpu
from jax.sharding import PartitionSpec as P

ITERS = 5


BETA = 0.9
DAMPING = 0.001
EPSILON = 1e-06


def batched(former, latter):
    return jnp.einsum(
        "kij,kjl->kil",
        former.astype(jnp.bfloat16),
        latter.astype(jnp.bfloat16),
        preferred_element_type=jnp.float32,
    )


def inverse_roots(stat_pair):
    identity = jnp.eye(stat_pair.shape[-1], dtype=jnp.float32)
    damped = stat_pair + DAMPING * identity
    frob_norm = jnp.sqrt(jnp.sum(damped * damped, axis=(1, 2), keepdims=True) + EPSILON)
    moment = damped / frob_norm
    result = jnp.broadcast_to(identity, stat_pair.shape)
    for iteration in range(ITERS):
        factor = (5.0 * identity - moment) * 0.25
        if iteration == 0:
            result = factor
        else:
            result = batched(result, factor)
        if iteration + 1 < ITERS:
            square = batched(factor, factor)
            moment = batched(square, batched(square, moment))
    return result * frob_norm ** (-0.25)


def precondition(grad_block, stat_pair):
    gram_left = lax.dot_general(
        grad_block, grad_block, (((1,), (1,)), ((), ())), preferred_element_type=jnp.float32
    )
    gram_right = lax.dot_general(
        grad_block, grad_block, (((0,), (0,)), ((), ())), preferred_element_type=jnp.float32
    )
    new_pair = BETA * stat_pair + (1.0 - BETA) * jnp.stack([gram_left, gram_right])
    root_pair = inverse_roots(new_pair)
    left_applied = jnp.dot(
        root_pair[0].astype(jnp.bfloat16), grad_block, preferred_element_type=jnp.float32
    )
    direction = jnp.dot(
        left_applied.astype(jnp.bfloat16),
        root_pair[1].astype(jnp.bfloat16),
        preferred_element_type=jnp.float32,
    )
    grad_wide = grad_block.astype(jnp.float32)
    graft_ratio = jnp.sqrt(
        (jnp.mean(grad_wide * grad_wide) + EPSILON) / (jnp.mean(direction * direction) + EPSILON)
    )
    return ((direction * graft_ratio).astype(jnp.bfloat16), new_pair)


def keep_slot(grad_block, stat_pair):
    return (jnp.zeros_like(grad_block), stat_pair)


def on_device(acts, cotangent, stats, owner_slot):
    dp_count = lax.axis_size("dp")
    my_index = lax.axis_index("dp")
    blk_size = cotangent.shape[1]
    blocks = acts.shape[1] // blk_size
    slot_count = stats.shape[1]
    piece_rows = blk_size // dp_count
    split_acts = acts.reshape(acts.shape[0], blocks, blk_size)
    my_slots = my_index * slot_count + jnp.arange(slot_count, dtype=jnp.int32)
    holds_block = owner_slot[None, :] == my_slots[:, None]
    filled = jnp.any(holds_block, axis=1)
    my_rows = lax.psum_scatter(
        jnp.einsum("twr,tc->rwc", split_acts, cotangent, preferred_element_type=jnp.float32),
        "dp",
        scatter_dimension=0,
        tiled=True,
    ).astype(jnp.bfloat16)
    slot_ids = jnp.arange(dp_count * slot_count, dtype=jnp.int32)
    selector = (owner_slot[None, :] == slot_ids[:, None]).astype(jnp.bfloat16)
    outgoing = jnp.einsum(
        "sw,rwc->src", selector, my_rows, preferred_element_type=jnp.float32
    ).astype(jnp.bfloat16)
    outgoing = outgoing.reshape(dp_count, slot_count, piece_rows, blk_size)
    arrived = lax.all_to_all(outgoing, "dp", split_axis=0, concat_axis=2, tiled=True)
    owned_grads = arrived.reshape(slot_count, blk_size, blk_size)
    slot_update, slot_stats = lax.cond(
        filled[0], precondition, keep_slot, owned_grads[0], stats[0, 0]
    )
    update_list = [slot_update]
    stat_list = [slot_stats]
    updates = jnp.stack(update_list)
    new_stats = jnp.stack(stat_list)[None]
    outgoing_rows = updates.reshape(slot_count, dp_count, piece_rows, blk_size)
    returned = lax.all_to_all(outgoing_rows, "dp", split_axis=1, concat_axis=1, tiled=True)
    grid_ids = (
        jnp.arange(slot_count, dtype=jnp.int32)[:, None]
        + slot_count * jnp.arange(dp_count, dtype=jnp.int32)[None, :]
    )
    picker = (owner_slot[:, None, None] == grid_ids[None]).astype(jnp.bfloat16)
    result = jnp.einsum(
        "wsn,snrc->wrc", picker, returned, preferred_element_type=jnp.float32
    ).astype(jnp.bfloat16)
    return (result, new_stats)


MESH = pl.DeviceIdType.MESH
LANES = 2
CHUNKS = 2


def gather_kernel(block_ref, acts_ref, cot_ref, grad_ref, stage, acts_all, cot_all, total,
                  a_send, a_recv, sib_send, sib_recv, y_send, y_recv, fwd_send, fwd_recv,
                  own_send, z_send, x_send, c_recv, load_sem, quarters, wholes):
    dp_count, tokens, blk = acts_all.shape
    mp_count = lax.axis_size("mp")
    part = tokens // mp_count
    chunk = tokens // CHUNKS
    depth = dp_count // LANES
    me = lax.axis_index("dp")
    mine = lax.axis_index("mp")
    z, x = me // LANES, me % LANES
    sibling = mine + 1 - 2 * (mine % 2)
    beside = (mine + 2) % mp_count
    my_rows = pl.ds(pl.multiple_of(mine * part, part), part)
    beside_rows = pl.ds(pl.multiple_of(beside * part, part), part)
    others = [(me + step) % dp_count for step in range(1, dp_count)]
    greeted = [(d, mine) for d in others] + [(me, sibling), (me, beside)]

    barrier = pltpu.get_barrier_semaphore()
    for d, m in greeted:
        pl.semaphore_signal(barrier, inc=1, device_id={"dp": d, "mp": m}, device_id_type=MESH)

    quarter_loads, whole_loads = [], []
    for w in range(dp_count):
        cols = pl.ds(w * blk, blk)
        quarter_loads.append(pltpu.make_async_copy(acts_ref.at[my_rows, cols], quarters.at[w], load_sem.at[0, w]))
        whole_loads.append(pltpu.make_async_copy(acts_ref.at[:, cols], wholes.at[w], load_sem.at[1, w]))
    for load in quarter_loads + whole_loads:
        load.start()
    for load in quarter_loads:
        load.wait()
    for d in range(dp_count):
        stage[d] = quarters[block_ref[d]]
    for load in whole_loads:
        load.wait()
    acts_all[me] = wholes[block_ref[me]]
    pl.semaphore_wait(barrier, len(greeted))

    def remote(src, dst, send, recv, d, m):
        return pltpu.make_async_remote_copy(
            src_ref=src, dst_ref=dst, send_sem=send, recv_sem=recv,
            device_id={"dp": d, "mp": m}, device_id_type=MESH)

    def acts_out(d):
        return remote(stage.at[d], acts_all.at[me, my_rows], a_send.at[d], a_recv.at[me], d, mine)

    def arrived(ref, sem):
        pltpu.make_async_copy(ref, ref, sem).wait()

    def rows_of(c):
        return pl.ds(c * chunk, chunk)

    def cot_piece(who, c):
        return cot_all.at[who, rows_of(c)]

    def own_out(way, c):
        target = (me + 1 - 2 * x, me + LANES, me - LANES)[way]
        return remote(cot_ref.at[rows_of(c)], cot_piece(me, c), own_send.at[way, c],
                      c_recv.at[me, c], target, mine)

    def z_out(zz, sign, c):
        who = zz * LANES + x
        return remote(cot_piece(who, c), cot_piece(who, c), z_send.at[zz, c], c_recv.at[who, c],
                      me + sign * LANES, mine)

    def x_out(zz, c):
        who = zz * LANES + x
        return remote(cot_piece(who, c), cot_piece(who, c), x_send.at[zz, c], c_recv.at[who, c],
                      me + 1 - 2 * x, mine)

    def side_out(s, which):
        if which == 0:
            return remote(acts_all.at[s, my_rows], acts_all.at[s, my_rows], sib_send.at[s],
                          sib_recv.at[s], me, sibling)
        if which == 1:
            return remote(acts_all.at[s, my_rows], acts_all.at[s, my_rows], y_send.at[s],
                          y_recv.at[s], me, beside)
        return remote(acts_all.at[s, beside_rows], acts_all.at[s, beside_rows], fwd_send.at[s],
                      fwd_recv.at[s], me, sibling)

    far_first = sorted(range(1, dp_count), key=lambda step: -min(step, dp_count - step))
    ordered = [(me + step) % dp_count for step in far_first]
    senders = [(me + dp_count - step) % dp_count for step in far_first]

    def own_everywhere(act):
        for c in range(CHUNKS):
            pl.when(z + 1 < depth)(lambda c=c: act(own_out(1, c)))
            pl.when(z > 0)(lambda c=c: act(own_out(2, c)))
            act(own_out(0, c))

    own_everywhere(lambda copy: copy.start())
    for d in ordered:
        acts_out(d).start()

    def relay(zz, sign, c):
        who = zz * LANES + x
        arrived(cot_piece(who, c), c_recv.at[who, c])
        nxt = z + sign
        pl.when(jnp.logical_and(nxt >= 0, nxt < depth))(lambda: z_out(zz, sign, c).start())
        x_out(zz, c).start()

    def relays(k):
        for c in range(CHUNKS):
            pl.when(z - k >= 0)(lambda c=c: relay(z - k, 1, c))
            pl.when(z + k < depth)(lambda c=c: relay(z + k, -1, c))

    def add_term(s, cot, first=False):
        term = lax.dot_general(acts_all[s], cot, (((0,), (0,)), ((), ())),
                               preferred_element_type=jnp.float32)
        total[...] = term if first else total[...] + term

    add_term(me, cot_ref[...], True)
    relays(1)
    for s in senders:
        arrived(acts_all.at[s, my_rows], a_recv.at[s])
        side_out(s, 0).start()
        side_out(s, 1).start()
    for k in range(2, depth):
        relays(k)
    for s in senders:
        arrived(acts_all.at[s, beside_rows], y_recv.at[s])
        side_out(s, 2).start()
    across = beside + 1 - 2 * (beside % 2)
    sibling_rows = pl.ds(pl.multiple_of(sibling * part, part), part)
    across_rows = pl.ds(pl.multiple_of(across * part, part), part)

    def acts_ready(s):
        arrived(acts_all.at[s, sibling_rows], sib_recv.at[s])
        arrived(acts_all.at[s, across_rows], fwd_recv.at[s])

    for k in range(1, depth):
        s = ((z + k) % depth) * LANES + x
        acts_ready(s)
        add_term(s, cot_all[s])
    for k in range(depth):
        s = ((z + k) % depth) * LANES + 1 - x
        acts_ready(s)
        for c in range(CHUNKS):
            arrived(cot_piece(s, c), c_recv.at[s, c])
        add_term(s, cot_all[s])
    grad_ref[...] = total[...].astype(grad_ref.dtype)

    own_everywhere(lambda copy: copy.wait_send())
    for d in ordered:
        acts_out(d).wait_send()
    for s in senders:
        for which in range(3):
            side_out(s, which).wait_send()

    def relay_sent(zz, sign, c):
        nxt = z + sign
        pl.when(jnp.logical_and(nxt >= 0, nxt < depth))(lambda: z_out(zz, sign, c).wait_send())
        x_out(zz, c).wait_send()

    for k in range(1, depth):
        for c in range(CHUNKS):
            pl.when(z - k >= 0)(lambda c=c, k=k: relay_sent(z - k, 1, c))
            pl.when(z + k < depth)(lambda c=c, k=k: relay_sent(z + k, -1, c))


def gather_gradient(slot_block, acts, cotangent, dp_count, mp_count):
    tokens, blk = cotangent.shape
    dma = pltpu.SemaphoreType.DMA
    depth = dp_count // LANES
    vmem = pl.BlockSpec(memory_space=pltpu.VMEM)
    return pl.pallas_call(
        gather_kernel,
        name="gather_gradient",
        out_shape=jax.ShapeDtypeStruct((blk, blk), jnp.bfloat16),
        in_specs=[pl.BlockSpec(memory_space=pltpu.SMEM), pl.BlockSpec(memory_space=pl.ANY), vmem],
        out_specs=vmem,
        scratch_shapes=[
            pltpu.VMEM((dp_count, tokens // mp_count, blk), jnp.bfloat16),
            pltpu.VMEM((dp_count, tokens, blk), jnp.bfloat16),
            pltpu.VMEM((dp_count, tokens, blk), jnp.bfloat16),
            pltpu.VMEM((blk, blk), jnp.float32),
        ] + [dma((dp_count,))] * 8 + [dma((3, CHUNKS)), dma((depth, CHUNKS)), dma((depth, CHUNKS)),
                                     dma((dp_count, CHUNKS)), dma((2, dp_count)),
                                     pltpu.VMEM((dp_count, tokens // mp_count, blk), jnp.bfloat16),
                                     pltpu.VMEM((dp_count, tokens, blk), jnp.bfloat16)],
        compiler_params=pltpu.CompilerParams(collective_id=0, has_side_effects=True),
    )(slot_block, acts, cotangent)


def mm(former, latter):
    return jnp.dot(former, latter, preferred_element_type=jnp.float32)


def root_kernel(grad_ref, stat_ref, dir_ref, new_ref):
    low = jnp.bfloat16
    blk = grad_ref.shape[0]
    grad = grad_ref[...]
    row = lax.broadcasted_iota(jnp.int32, (blk, blk), 0)
    col = lax.broadcasted_iota(jnp.int32, (blk, blk), 1)
    diagonal = row == col
    grams = [
        lax.dot_general(grad, grad, (((1,), (1,)), ((), ())), preferred_element_type=jnp.float32),
        lax.dot_general(grad, grad, (((0,), (0,)), ((), ())), preferred_element_type=jnp.float32),
    ]
    moments, results, scales = [], [None, None], []
    for side in range(2):
        fresh = BETA * stat_ref[side] + (1.0 - BETA) * grams[side]
        new_ref[side] = fresh
        damped = fresh + jnp.where(diagonal, DAMPING, 0.0)
        frob = jnp.sqrt(jnp.sum(damped * damped, axis=(0, 1), keepdims=True) + EPSILON)
        scales.append(lax.rsqrt(jnp.sqrt(frob)))
        moments.append(damped * (1.0 / frob))
    for iteration in range(ITERS):
        factors = [(jnp.where(diagonal, 5.0, 0.0) - moments[side]) * 0.25 for side in range(2)]
        lows = [factors[side].astype(low) for side in range(2)]
        if iteration + 1 < ITERS:
            squares = [mm(lows[side], lows[side]).astype(low) for side in range(2)]
            inner = [mm(squares[side], moments[side].astype(low)).astype(low) for side in range(2)]
            moments = [mm(squares[side], inner[side]) for side in range(2)]
        for side in range(2):
            results[side] = factors[side] if iteration == 0 else mm(results[side].astype(low), lows[side])
    roots = [(results[side] * scales[side]).astype(low) for side in range(2)]
    direction = mm(mm(roots[0], grad).astype(low), roots[1])
    wide = grad.astype(jnp.float32)
    count = blk * blk
    power = jnp.sum(wide * wide, axis=(0, 1), keepdims=True) / count + EPSILON
    reached = jnp.sum(direction * direction, axis=(0, 1), keepdims=True) / count + EPSILON
    dir_ref[...] = (direction * jnp.sqrt(power / reached)).astype(low)


def apply_roots(grad, stat_pair):
    vmem = pl.BlockSpec(memory_space=pltpu.VMEM)
    return pl.pallas_call(
        root_kernel,
        name="apply_roots",
        out_shape=(jax.ShapeDtypeStruct(grad.shape, jnp.bfloat16),
                   jax.ShapeDtypeStruct(stat_pair.shape, jnp.float32)),
        in_specs=[vmem, vmem],
        out_specs=(vmem, vmem),
    )(grad, stat_pair)


def return_kernel(owner_ref, dir_ref, out_ref, held, send, recv):
    dp_count, piece, blk = held.shape
    me = lax.axis_index("dp")
    others = [(me + step) % dp_count for step in range(1, dp_count)]
    barrier = pltpu.get_barrier_semaphore()
    for d in others:
        pl.semaphore_signal(barrier, inc=1, device_id={"dp": d}, device_id_type=MESH)
    pl.semaphore_wait(barrier, len(others))

    def rows_of(d):
        return pl.ds(pl.multiple_of(d * piece, piece), piece)

    far_first = sorted(range(1, dp_count), key=lambda step: -min(step, dp_count - step))
    copies = []
    for step in far_first:
        d = (me + step) % dp_count
        copy = pltpu.make_async_remote_copy(
            src_ref=dir_ref.at[rows_of(d)], dst_ref=held.at[me], send_sem=send.at[d],
            recv_sem=recv.at[me], device_id={"dp": d}, device_id_type=MESH)
        copy.start()
        copies.append(copy)
    held[me] = dir_ref[rows_of(me)]
    for d in others:
        pltpu.make_async_copy(held.at[d], held.at[d], recv.at[d]).wait()
    for w in range(dp_count):
        out_ref[w] = held[owner_ref[w]]
    for copy in copies:
        copy.wait_send()


def return_rows(owner_slot, direction, dp_count):
    blk = direction.shape[0]
    shape = (dp_count, blk // dp_count, blk)
    vmem = pl.BlockSpec(memory_space=pltpu.VMEM)
    dma = pltpu.SemaphoreType.DMA
    return pl.pallas_call(
        return_kernel,
        name="return_rows",
        out_shape=jax.ShapeDtypeStruct(shape, jnp.bfloat16),
        in_specs=[pl.BlockSpec(memory_space=pltpu.SMEM), vmem],
        out_specs=vmem,
        scratch_shapes=[pltpu.VMEM(shape, jnp.bfloat16), dma((dp_count,)), dma((dp_count,))],
        compiler_params=pltpu.CompilerParams(collective_id=1, has_side_effects=True),
    )(owner_slot, direction)


def full_house(acts, cotangent, stats, owner_slot):
    dp_count, mp_count = lax.axis_size("dp"), lax.axis_size("mp")
    ids = jnp.arange(dp_count, dtype=jnp.int32)
    slot_block = jnp.sum(jnp.where(owner_slot[None, :] == ids[:, None], ids[None, :], 0), axis=1)
    grad = gather_gradient(slot_block, acts, cotangent, dp_count, mp_count)
    direction, new_pair = apply_roots(grad, stats[0, 0])
    return return_rows(owner_slot, direction, dp_count), new_pair[None, None]


def device_body(acts, cotangent, stats, owner_slot):
    dp_count, mp_count = lax.axis_size("dp"), lax.axis_size("mp")
    blk = cotangent.shape[1]
    every_slot_filled = stats.shape[1] == 1 and acts.shape[1] == dp_count * blk
    if every_slot_filled and mp_count == 4 and dp_count % LANES == 0 and dp_count <= 8:
        return full_house(acts, cotangent, stats, owner_slot)
    return on_device(acts, cotangent, stats, owner_slot)


def solution(mesh):
    return jax.shard_map(
        device_body,
        mesh=mesh,
        in_specs=(P("dp", None), P("dp", "mp"), P("mp", "dp", None, None, None), P()),
        out_specs=(P(None, "dp", "mp"), P("mp", "dp", None, None, None)),
        check_vma=False,
    )
```

```python
import jax
import jax.numpy as jnp
from jax import lax
from jax.experimental import pallas as pl
from jax.experimental.pallas import tpu as pltpu
from jax.sharding import PartitionSpec as P

ITERS = 5


BETA = 0.9
DAMPING = 0.001
EPSILON = 1e-06


def batched(former, latter):
    return jnp.einsum(
        "kij,kjl->kil",
        former.astype(jnp.bfloat16),
        latter.astype(jnp.bfloat16),
        preferred_element_type=jnp.float32,
    )


def inverse_roots(stat_pair):
    identity = jnp.eye(stat_pair.shape[-1], dtype=jnp.float32)
    damped = stat_pair + DAMPING * identity
    frob_norm = jnp.sqrt(jnp.sum(damped * damped, axis=(1, 2), keepdims=True) + EPSILON)
    moment = damped / frob_norm
    result = jnp.broadcast_to(identity, stat_pair.shape)
    for iteration in range(ITERS):
        factor = (5.0 * identity - moment) * 0.25
        if iteration == 0:
            result = factor
        else:
            result = batched(result, factor)
        if iteration + 1 < ITERS:
            square = batched(factor, factor)
            moment = batched(square, batched(square, moment))
    return result * frob_norm ** (-0.25)


def precondition(grad_block, stat_pair):
    gram_left = lax.dot_general(
        grad_block, grad_block, (((1,), (1,)), ((), ())), preferred_element_type=jnp.float32
    )
    gram_right = lax.dot_general(
        grad_block, grad_block, (((0,), (0,)), ((), ())), preferred_element_type=jnp.float32
    )
    new_pair = BETA * stat_pair + (1.0 - BETA) * jnp.stack([gram_left, gram_right])
    root_pair = inverse_roots(new_pair)
    left_applied = jnp.dot(
        root_pair[0].astype(jnp.bfloat16), grad_block, preferred_element_type=jnp.float32
    )
    direction = jnp.dot(
        left_applied.astype(jnp.bfloat16),
        root_pair[1].astype(jnp.bfloat16),
        preferred_element_type=jnp.float32,
    )
    grad_wide = grad_block.astype(jnp.float32)
    graft_ratio = jnp.sqrt(
        (jnp.mean(grad_wide * grad_wide) + EPSILON) / (jnp.mean(direction * direction) + EPSILON)
    )
    return ((direction * graft_ratio).astype(jnp.bfloat16), new_pair)


def keep_slot(grad_block, stat_pair):
    return (jnp.zeros_like(grad_block), stat_pair)


def on_device(acts, cotangent, stats, owner_slot):
    dp_count = lax.axis_size("dp")
    my_index = lax.axis_index("dp")
    blk_size = cotangent.shape[1]
    blocks = acts.shape[1] // blk_size
    slot_count = stats.shape[1]
    piece_rows = blk_size // dp_count
    split_acts = acts.reshape(acts.shape[0], blocks, blk_size)
    my_slots = my_index * slot_count + jnp.arange(slot_count, dtype=jnp.int32)
    holds_block = owner_slot[None, :] == my_slots[:, None]
    filled = jnp.any(holds_block, axis=1)
    my_rows = lax.psum_scatter(
        jnp.einsum("twr,tc->rwc", split_acts, cotangent, preferred_element_type=jnp.float32),
        "dp",
        scatter_dimension=0,
        tiled=True,
    ).astype(jnp.bfloat16)
    slot_ids = jnp.arange(dp_count * slot_count, dtype=jnp.int32)
    selector = (owner_slot[None, :] == slot_ids[:, None]).astype(jnp.bfloat16)
    outgoing = jnp.einsum(
        "sw,rwc->src", selector, my_rows, preferred_element_type=jnp.float32
    ).astype(jnp.bfloat16)
    outgoing = outgoing.reshape(dp_count, slot_count, piece_rows, blk_size)
    arrived = lax.all_to_all(outgoing, "dp", split_axis=0, concat_axis=2, tiled=True)
    owned_grads = arrived.reshape(slot_count, blk_size, blk_size)
    slot_update, slot_stats = lax.cond(
        filled[0], precondition, keep_slot, owned_grads[0], stats[0, 0]
    )
    update_list = [slot_update]
    stat_list = [slot_stats]
    updates = jnp.stack(update_list)
    new_stats = jnp.stack(stat_list)[None]
    outgoing_rows = updates.reshape(slot_count, dp_count, piece_rows, blk_size)
    returned = lax.all_to_all(outgoing_rows, "dp", split_axis=1, concat_axis=1, tiled=True)
    grid_ids = (
        jnp.arange(slot_count, dtype=jnp.int32)[:, None]
        + slot_count * jnp.arange(dp_count, dtype=jnp.int32)[None, :]
    )
    picker = (owner_slot[:, None, None] == grid_ids[None]).astype(jnp.bfloat16)
    result = jnp.einsum(
        "wsn,snrc->wrc", picker, returned, preferred_element_type=jnp.float32
    ).astype(jnp.bfloat16)
    return (result, new_stats)


MESH = pl.DeviceIdType.MESH
LANES = 2
CHUNKS = 4


def gather_kernel(owner_ref, acts_ref, cot_ref, grad_ref, stage, acts_all, cot_all, total,
                  a_send, a_recv, sib_send, sib_recv, y_send, y_recv, fwd_send, fwd_recv,
                  own_send, z_send, x_send, c_recv, load_sem, quarters, wholes):
    dp_count, tokens, blk = acts_all.shape
    mp_count = lax.axis_size("mp")
    part = tokens // mp_count
    chunk = tokens // CHUNKS
    depth = dp_count // LANES
    me = lax.axis_index("dp")
    mine = lax.axis_index("mp")
    z, x = me // LANES, me % LANES
    sibling = mine + 1 - 2 * (mine % 2)
    beside = (mine + 2) % mp_count
    my_rows = pl.ds(pl.multiple_of(mine * part, part), part)
    beside_rows = pl.ds(pl.multiple_of(beside * part, part), part)
    others = [(me + step) % dp_count for step in range(1, dp_count)]
    greeted = [(d, mine) for d in others] + [(me, sibling), (me, beside)]

    quarter_loads, whole_loads = [], []
    for w in range(dp_count):
        cols = pl.ds(w * blk, blk)
        quarter_loads.append(pltpu.make_async_copy(acts_ref.at[my_rows, cols], quarters.at[w], load_sem.at[0, w]))
        whole_loads.append(pltpu.make_async_copy(acts_ref.at[:, cols], wholes.at[w], load_sem.at[1, w]))
    for load in quarter_loads + whole_loads:
        load.start()
    barrier = pltpu.get_barrier_semaphore()
    for d, m in greeted:
        pl.semaphore_signal(barrier, inc=1, device_id={"dp": d, "mp": m}, device_id_type=MESH)

    def remote(src, dst, send, recv, d, m):
        return pltpu.make_async_remote_copy(
            src_ref=src, dst_ref=dst, send_sem=send, recv_sem=recv,
            device_id={"dp": d, "mp": m}, device_id_type=MESH)

    def acts_out(d):
        return remote(stage.at[d], acts_all.at[me, my_rows], a_send.at[d], a_recv.at[me], d, mine)

    def arrived(ref, sem):
        pltpu.make_async_copy(ref, ref, sem).wait()

    def rows_of(c):
        return pl.ds(c * chunk, chunk)

    def cot_piece(who, c):
        return cot_all.at[who, rows_of(c)]

    def own_out(way, c):
        target = (me + 1 - 2 * x, me + LANES, me - LANES)[way]
        return remote(cot_ref.at[rows_of(c)], cot_piece(me, c), own_send.at[way, c],
                      c_recv.at[me, c], target, mine)

    def z_out(zz, sign, c):
        who = zz * LANES + x
        return remote(cot_piece(who, c), cot_piece(who, c), z_send.at[zz, c], c_recv.at[who, c],
                      me + sign * LANES, mine)

    def x_out(zz, c):
        who = zz * LANES + x
        return remote(cot_piece(who, c), cot_piece(who, c), x_send.at[zz, c], c_recv.at[who, c],
                      me + 1 - 2 * x, mine)

    def side_out(s, which):
        if which == 0:
            return remote(acts_all.at[s, my_rows], acts_all.at[s, my_rows], sib_send.at[s],
                          sib_recv.at[s], me, sibling)
        if which == 1:
            return remote(acts_all.at[s, my_rows], acts_all.at[s, my_rows], y_send.at[s],
                          y_recv.at[s], me, beside)
        return remote(acts_all.at[s, beside_rows], acts_all.at[s, beside_rows], fwd_send.at[s],
                      fwd_recv.at[s], me, sibling)

    far_first = sorted(range(1, dp_count), key=lambda step: -min(step, dp_count - step))
    ordered = [(me + step) % dp_count for step in far_first]
    senders = [(me + dp_count - step) % dp_count for step in far_first]

    def own_everywhere(act):
        for c in range(CHUNKS):
            pl.when(z + 1 < depth)(lambda c=c: act(own_out(1, c)))
            pl.when(z > 0)(lambda c=c: act(own_out(2, c)))
            act(own_out(0, c))

    def block_at(slot):
        found = 0
        for w in range(1, dp_count):
            gap = owner_ref[w] - slot
            found = found + w * jnp.maximum(1 - gap * gap, 0)
        return jnp.minimum(found, dp_count - 1)

    pl.semaphore_wait(barrier, len(greeted))
    own_everywhere(lambda copy: copy.start())
    for load in quarter_loads:
        load.wait()
    for d in range(dp_count):
        stage[d] = quarters[block_at(d)]
    for load in whole_loads:
        load.wait()
    acts_all[me] = wholes[block_at(me)]


    def relay(zz, sign, c):
        who = zz * LANES + x
        arrived(cot_piece(who, c), c_recv.at[who, c])
        nxt = z + sign
        pl.when(jnp.logical_and(nxt >= 0, nxt < depth))(lambda: z_out(zz, sign, c).start())
        x_out(zz, c).start()

    def relays(k):
        for c in range(CHUNKS):
            pl.when(z - k >= 0)(lambda c=c: relay(z - k, 1, c))
            pl.when(z + k < depth)(lambda c=c: relay(z + k, -1, c))

    def add_term(s, cot, first=False):
        term = lax.dot_general(acts_all[s], cot, (((0,), (0,)), ((), ())),
                               preferred_element_type=jnp.float32)
        total[...] = term if first else total[...] + term

    across = beside + 1 - 2 * (beside % 2)
    sibling_rows = pl.ds(pl.multiple_of(sibling * part, part), part)
    across_rows = pl.ds(pl.multiple_of(across * part, part), part)

    def acts_ready(s):
        arrived(acts_all.at[s, sibling_rows], sib_recv.at[s])
        arrived(acts_all.at[s, across_rows], fwd_recv.at[s])

    add_term(me, cot_ref[...], True)
    for k in range(1, depth):
        relays(k)
        if k == max(depth - 2, 1):
            for d in ordered:
                acts_out(d).start()

    inward = 1 - 2 * (2 * z // depth)
    arrivals = [(True, z * LANES + 1 - x)]
    for k in range(1, depth):
        zz = (z + inward * k + depth) % depth
        arrivals += [(False, zz * LANES + x), (True, zz * LANES + 1 - x)]
    for i in range(len(arrivals) + 2):
        if i < len(arrivals):
            s = arrivals[i][1]
            arrived(acts_all.at[s, my_rows], a_recv.at[s])
            side_out(s, 0).start()
            side_out(s, 1).start()
        if 1 <= i <= len(arrivals):
            s = arrivals[i - 1][1]
            arrived(acts_all.at[s, beside_rows], y_recv.at[s])
            side_out(s, 2).start()
        if i >= 2 and not arrivals[i - 2][0]:
            s = arrivals[i - 2][1]
            acts_ready(s)
            add_term(s, cot_all[s])
    for is_beside, s in arrivals:
        if is_beside:
            acts_ready(s)
            for c in range(CHUNKS):
                arrived(cot_piece(s, c), c_recv.at[s, c])
            add_term(s, cot_all[s])
    grad_ref[...] = total[...].astype(grad_ref.dtype)

    own_everywhere(lambda copy: copy.wait_send())
    for d in ordered:
        acts_out(d).wait_send()
    for s in senders:
        for which in range(3):
            side_out(s, which).wait_send()

    def relay_sent(zz, sign, c):
        nxt = z + sign
        pl.when(jnp.logical_and(nxt >= 0, nxt < depth))(lambda: z_out(zz, sign, c).wait_send())
        x_out(zz, c).wait_send()

    for k in range(1, depth):
        for c in range(CHUNKS):
            pl.when(z - k >= 0)(lambda c=c, k=k: relay_sent(z - k, 1, c))
            pl.when(z + k < depth)(lambda c=c, k=k: relay_sent(z + k, -1, c))


def gather_gradient(owner_slot, acts, cotangent, dp_count, mp_count):
    tokens, blk = cotangent.shape
    dma = pltpu.SemaphoreType.DMA
    depth = dp_count // LANES
    vmem = pl.BlockSpec(memory_space=pltpu.VMEM)
    return pl.pallas_call(
        gather_kernel,
        name="gather_gradient",
        out_shape=jax.ShapeDtypeStruct((blk, blk), jnp.bfloat16),
        in_specs=[pl.BlockSpec(memory_space=pltpu.SMEM), pl.BlockSpec(memory_space=pl.ANY), vmem],
        out_specs=vmem,
        scratch_shapes=[
            pltpu.VMEM((dp_count, tokens // mp_count, blk), jnp.bfloat16),
            pltpu.VMEM((dp_count, tokens, blk), jnp.bfloat16),
            pltpu.VMEM((dp_count, tokens, blk), jnp.bfloat16),
            pltpu.VMEM((blk, blk), jnp.float32),
        ] + [dma((dp_count,))] * 8 + [dma((3, CHUNKS)), dma((depth, CHUNKS)), dma((depth, CHUNKS)),
                                     dma((dp_count, CHUNKS)), dma((2, dp_count)),
                                     pltpu.VMEM((dp_count, tokens // mp_count, blk), jnp.bfloat16),
                                     pltpu.VMEM((dp_count, tokens, blk), jnp.bfloat16)],
        compiler_params=pltpu.CompilerParams(collective_id=0, has_side_effects=True),
    )(owner_slot, acts, cotangent)


def mm(former, latter):
    return jnp.dot(former, latter, preferred_element_type=jnp.float32)


def root_kernel(grad_ref, stat_any, dir_ref, new_any, stat_ref, new_ref, in_sem, out_sem):
    low = jnp.bfloat16
    blk = grad_ref.shape[0]
    loads = [pltpu.make_async_copy(stat_any.at[k], stat_ref.at[k], in_sem.at[k]) for k in range(2)]
    stores = [pltpu.make_async_copy(new_ref.at[k], new_any.at[k], out_sem.at[k]) for k in range(2)]
    for load in loads:
        load.start()
    grad = grad_ref[...]
    row = lax.broadcasted_iota(jnp.int32, (blk, blk), 0)
    col = lax.broadcasted_iota(jnp.int32, (blk, blk), 1)
    diagonal = row == col
    grams = [
        lax.dot_general(grad, grad, (((1,), (1,)), ((), ())), preferred_element_type=jnp.float32),
        lax.dot_general(grad, grad, (((0,), (0,)), ((), ())), preferred_element_type=jnp.float32),
    ]
    moments, results, scales = [], [None, None], []
    for side in range(2):
        loads[side].wait()
        fresh = BETA * stat_ref[side] + (1.0 - BETA) * grams[side]
        new_ref[side] = fresh
        stores[side].start()
        damped = fresh + jnp.where(diagonal, DAMPING, 0.0)
        frob = jnp.sqrt(jnp.sum(damped * damped, axis=(0, 1), keepdims=True) + EPSILON)
        scales.append(lax.rsqrt(jnp.sqrt(frob)))
        moments.append(damped * (1.0 / frob))
    for iteration in range(ITERS):
        factors = [(jnp.where(diagonal, 5.0, 0.0) - moments[side]) * 0.25 for side in range(2)]
        lows = [factors[side].astype(low) for side in range(2)]
        if iteration + 1 < ITERS:
            squares = [mm(lows[side], lows[side]).astype(low) for side in range(2)]
            inner = [mm(squares[side], moments[side].astype(low)).astype(low) for side in range(2)]
            moments = [mm(squares[side], inner[side]) for side in range(2)]
        for side in range(2):
            results[side] = factors[side] if iteration == 0 else mm(results[side].astype(low), lows[side])
    roots = [(results[side] * scales[side]).astype(low) for side in range(2)]
    direction = mm(mm(roots[0], grad).astype(low), roots[1])
    wide = grad.astype(jnp.float32)
    count = blk * blk
    power = jnp.sum(wide * wide, axis=(0, 1), keepdims=True) / count + EPSILON
    reached = jnp.sum(direction * direction, axis=(0, 1), keepdims=True) / count + EPSILON
    dir_ref[...] = (direction * jnp.sqrt(power / reached)).astype(low)
    for store in stores:
        store.wait()


def apply_roots(grad, stat_pair):
    vmem = pl.BlockSpec(memory_space=pltpu.VMEM)
    return pl.pallas_call(
        root_kernel,
        name="apply_roots",
        out_shape=(jax.ShapeDtypeStruct(grad.shape, jnp.bfloat16),
                   jax.ShapeDtypeStruct(stat_pair.shape, jnp.float32)),
        in_specs=[vmem, pl.BlockSpec(memory_space=pl.ANY)],
        out_specs=(vmem, pl.BlockSpec(memory_space=pl.ANY)),
        scratch_shapes=[pltpu.VMEM(stat_pair.shape, jnp.float32)] * 2
        + [pltpu.SemaphoreType.DMA((2,))] * 2,
    )(grad, stat_pair)


def return_kernel(owner_ref, dir_ref, out_ref, held, send, recv):
    dp_count, piece, blk = held.shape
    me = lax.axis_index("dp")
    others = [(me + step) % dp_count for step in range(1, dp_count)]
    barrier = pltpu.get_barrier_semaphore()
    for d in others:
        pl.semaphore_signal(barrier, inc=1, device_id={"dp": d}, device_id_type=MESH)
    pl.semaphore_wait(barrier, len(others))

    def rows_of(d):
        return pl.ds(pl.multiple_of(d * piece, piece), piece)

    far_first = sorted(range(1, dp_count), key=lambda step: -min(step, dp_count - step))
    copies = []
    for step in far_first:
        d = (me + step) % dp_count
        copy = pltpu.make_async_remote_copy(
            src_ref=dir_ref.at[rows_of(d)], dst_ref=held.at[me], send_sem=send.at[d],
            recv_sem=recv.at[me], device_id={"dp": d}, device_id_type=MESH)
        copy.start()
        copies.append(copy)
    held[me] = dir_ref[rows_of(me)]
    for d in others:
        pltpu.make_async_copy(held.at[d], held.at[d], recv.at[d]).wait()
    for w in range(dp_count):
        out_ref[w] = held[owner_ref[w]]
    for copy in copies:
        copy.wait_send()


def return_rows(owner_slot, direction, dp_count):
    blk = direction.shape[0]
    shape = (dp_count, blk // dp_count, blk)
    vmem = pl.BlockSpec(memory_space=pltpu.VMEM)
    dma = pltpu.SemaphoreType.DMA
    return pl.pallas_call(
        return_kernel,
        name="return_rows",
        out_shape=jax.ShapeDtypeStruct(shape, jnp.bfloat16),
        in_specs=[pl.BlockSpec(memory_space=pltpu.SMEM), vmem],
        out_specs=vmem,
        scratch_shapes=[pltpu.VMEM(shape, jnp.bfloat16), dma((dp_count,)), dma((dp_count,))],
        compiler_params=pltpu.CompilerParams(collective_id=1, has_side_effects=True),
    )(owner_slot, direction)


def full_house(acts, cotangent, stats, owner_slot):
    dp_count, mp_count = lax.axis_size("dp"), lax.axis_size("mp")
    grad = gather_gradient(owner_slot, acts, cotangent, dp_count, mp_count)
    direction, new_pair = apply_roots(grad, stats[0, 0])
    return return_rows(owner_slot, direction, dp_count), new_pair[None, None]


def device_body(acts, cotangent, stats, owner_slot):
    dp_count, mp_count = lax.axis_size("dp"), lax.axis_size("mp")
    blk = cotangent.shape[1]
    every_slot_filled = stats.shape[1] == 1 and acts.shape[1] == dp_count * blk
    if every_slot_filled and mp_count == 4 and dp_count % LANES == 0 and dp_count <= 8:
        return full_house(acts, cotangent, stats, owner_slot)
    return on_device(acts, cotangent, stats, owner_slot)


def solution(mesh):
    return jax.shard_map(
        device_body,
        mesh=mesh,
        in_specs=(P("dp", None), P("dp", "mp"), P("mp", "dp", None, None, None), P()),
        out_specs=(P(None, "dp", "mp"), P("mp", "dp", None, None, None)),
        check_vma=False,
    )
```

```python
import jax
import jax.numpy as jnp
from jax import lax
from jax.experimental import pallas as pl
from jax.experimental.pallas import tpu as pltpu
from jax.sharding import PartitionSpec as P

ITERS = 5


BETA = 0.9
DAMPING = 0.001
EPSILON = 1e-06


def batched(former, latter):
    return jnp.einsum(
        "kij,kjl->kil",
        former.astype(jnp.bfloat16),
        latter.astype(jnp.bfloat16),
        preferred_element_type=jnp.float32,
    )


def inverse_roots(stat_pair):
    identity = jnp.eye(stat_pair.shape[-1], dtype=jnp.float32)
    damped = stat_pair + DAMPING * identity
    frob_norm = jnp.sqrt(jnp.sum(damped * damped, axis=(1, 2), keepdims=True) + EPSILON)
    moment = damped / frob_norm
    result = jnp.broadcast_to(identity, stat_pair.shape)
    for iteration in range(ITERS):
        factor = (5.0 * identity - moment) * 0.25
        if iteration == 0:
            result = factor
        else:
            result = batched(result, factor)
        if iteration + 1 < ITERS:
            square = batched(factor, factor)
            moment = batched(square, batched(square, moment))
    return result * frob_norm ** (-0.25)


def precondition(grad_block, stat_pair):
    gram_left = lax.dot_general(
        grad_block, grad_block, (((1,), (1,)), ((), ())), preferred_element_type=jnp.float32
    )
    gram_right = lax.dot_general(
        grad_block, grad_block, (((0,), (0,)), ((), ())), preferred_element_type=jnp.float32
    )
    new_pair = BETA * stat_pair + (1.0 - BETA) * jnp.stack([gram_left, gram_right])
    root_pair = inverse_roots(new_pair)
    left_applied = jnp.dot(
        root_pair[0].astype(jnp.bfloat16), grad_block, preferred_element_type=jnp.float32
    )
    direction = jnp.dot(
        left_applied.astype(jnp.bfloat16),
        root_pair[1].astype(jnp.bfloat16),
        preferred_element_type=jnp.float32,
    )
    grad_wide = grad_block.astype(jnp.float32)
    graft_ratio = jnp.sqrt(
        (jnp.mean(grad_wide * grad_wide) + EPSILON) / (jnp.mean(direction * direction) + EPSILON)
    )
    return ((direction * graft_ratio).astype(jnp.bfloat16), new_pair)


def keep_slot(grad_block, stat_pair):
    return (jnp.zeros_like(grad_block), stat_pair)


def on_device(acts, cotangent, stats, owner_slot):
    dp_count = lax.axis_size("dp")
    my_index = lax.axis_index("dp")
    blk_size = cotangent.shape[1]
    blocks = acts.shape[1] // blk_size
    slot_count = stats.shape[1]
    piece_rows = blk_size // dp_count
    split_acts = acts.reshape(acts.shape[0], blocks, blk_size)
    my_slots = my_index * slot_count + jnp.arange(slot_count, dtype=jnp.int32)
    holds_block = owner_slot[None, :] == my_slots[:, None]
    filled = jnp.any(holds_block, axis=1)
    my_rows = lax.psum_scatter(
        jnp.einsum("twr,tc->rwc", split_acts, cotangent, preferred_element_type=jnp.float32),
        "dp",
        scatter_dimension=0,
        tiled=True,
    ).astype(jnp.bfloat16)
    slot_ids = jnp.arange(dp_count * slot_count, dtype=jnp.int32)
    selector = (owner_slot[None, :] == slot_ids[:, None]).astype(jnp.bfloat16)
    outgoing = jnp.einsum(
        "sw,rwc->src", selector, my_rows, preferred_element_type=jnp.float32
    ).astype(jnp.bfloat16)
    outgoing = outgoing.reshape(dp_count, slot_count, piece_rows, blk_size)
    arrived = lax.all_to_all(outgoing, "dp", split_axis=0, concat_axis=2, tiled=True)
    owned_grads = arrived.reshape(slot_count, blk_size, blk_size)
    slot_update, slot_stats = lax.cond(
        filled[0], precondition, keep_slot, owned_grads[0], stats[0, 0]
    )
    update_list = [slot_update]
    stat_list = [slot_stats]
    updates = jnp.stack(update_list)
    new_stats = jnp.stack(stat_list)[None]
    outgoing_rows = updates.reshape(slot_count, dp_count, piece_rows, blk_size)
    returned = lax.all_to_all(outgoing_rows, "dp", split_axis=1, concat_axis=1, tiled=True)
    grid_ids = (
        jnp.arange(slot_count, dtype=jnp.int32)[:, None]
        + slot_count * jnp.arange(dp_count, dtype=jnp.int32)[None, :]
    )
    picker = (owner_slot[:, None, None] == grid_ids[None]).astype(jnp.bfloat16)
    result = jnp.einsum(
        "wsn,snrc->wrc", picker, returned, preferred_element_type=jnp.float32
    ).astype(jnp.bfloat16)
    return (result, new_stats)


MESH = pl.DeviceIdType.MESH
LANES = 2
CHUNKS = 2


def gather_kernel(owner_ref, acts_ref, cot_ref, grad_ref, stage, acts_all, cot_all, total,
                  a_send, a_recv, sib_send, sib_recv, y_send, y_recv, fwd_send, fwd_recv,
                  own_send, z_send, x_send, c_recv, load_sem, quarters, wholes):
    dp_count, tokens, blk = acts_all.shape
    mp_count = lax.axis_size("mp")
    part = tokens // mp_count
    chunk = tokens // CHUNKS
    depth = dp_count // LANES
    me = lax.axis_index("dp")
    mine = lax.axis_index("mp")
    z, x = me // LANES, me % LANES
    sibling = mine + 1 - 2 * (mine % 2)
    beside = (mine + 2) % mp_count
    my_rows = pl.ds(pl.multiple_of(mine * part, part), part)
    beside_rows = pl.ds(pl.multiple_of(beside * part, part), part)
    others = [(me + step) % dp_count for step in range(1, dp_count)]
    greeted = [(d, mine) for d in others] + [(me, sibling), (me, beside)]

    quarter_loads, whole_loads = [], []
    for w in range(dp_count):
        cols = pl.ds(w * blk, blk)
        quarter_loads.append(pltpu.make_async_copy(acts_ref.at[my_rows, cols], quarters.at[w], load_sem.at[0, w]))
        whole_loads.append(pltpu.make_async_copy(acts_ref.at[:, cols], wholes.at[w], load_sem.at[1, w]))
    for load in quarter_loads + whole_loads:
        load.start()
    barrier = pltpu.get_barrier_semaphore()
    for d, m in greeted:
        pl.semaphore_signal(barrier, inc=1, device_id={"dp": d, "mp": m}, device_id_type=MESH)

    def remote(src, dst, send, recv, d, m):
        return pltpu.make_async_remote_copy(
            src_ref=src, dst_ref=dst, send_sem=send, recv_sem=recv,
            device_id={"dp": d, "mp": m}, device_id_type=MESH)

    def acts_out(d):
        return remote(stage.at[d], acts_all.at[me, my_rows], a_send.at[d], a_recv.at[me], d, mine)

    def arrived(ref, sem):
        pltpu.make_async_copy(ref, ref, sem).wait()

    def rows_of(c):
        return pl.ds(c * chunk, chunk)

    def cot_piece(who, c):
        return cot_all.at[who, rows_of(c)]

    def own_out(way, c):
        target = (me + 1 - 2 * x, me + LANES, me - LANES)[way]
        return remote(cot_ref.at[rows_of(c)], cot_piece(me, c), own_send.at[way, c],
                      c_recv.at[me, c], target, mine)

    def z_out(zz, sign, c):
        who = zz * LANES + x
        return remote(cot_piece(who, c), cot_piece(who, c), z_send.at[zz, c], c_recv.at[who, c],
                      me + sign * LANES, mine)

    def x_out(zz, c):
        who = zz * LANES + x
        return remote(cot_piece(who, c), cot_piece(who, c), x_send.at[zz, c], c_recv.at[who, c],
                      me + 1 - 2 * x, mine)

    def side_out(s, which):
        if which == 0:
            return remote(acts_all.at[s, my_rows], acts_all.at[s, my_rows], sib_send.at[s],
                          sib_recv.at[s], me, sibling)
        if which == 1:
            return remote(acts_all.at[s, my_rows], acts_all.at[s, my_rows], y_send.at[s],
                          y_recv.at[s], me, beside)
        return remote(acts_all.at[s, beside_rows], acts_all.at[s, beside_rows], fwd_send.at[s],
                      fwd_recv.at[s], me, sibling)

    far_first = sorted(range(1, dp_count), key=lambda step: -min(step, dp_count - step))
    ordered = [(me + step) % dp_count for step in far_first]
    senders = [(me + dp_count - step) % dp_count for step in far_first]

    def own_everywhere(act):
        for c in range(CHUNKS):
            pl.when(z + 1 < depth)(lambda c=c: act(own_out(1, c)))
            pl.when(z > 0)(lambda c=c: act(own_out(2, c)))
            act(own_out(0, c))

    def block_at(slot):
        found = 0
        for w in range(1, dp_count):
            gap = owner_ref[w] - slot
            found = found + w * jnp.maximum(1 - gap * gap, 0)
        return jnp.minimum(found, dp_count - 1)

    inward = 1 - 2 * (2 * z // depth)
    arrivals = [(True, z * LANES + 1 - x)]
    for k in range(1, depth):
        zz = (z + inward * k + depth) % depth
        arrivals += [(False, zz * LANES + x), (True, zz * LANES + 1 - x)]
    for load in quarter_loads:
        load.wait()
    for d in range(dp_count):
        stage[d] = quarters[block_at(d)]
    pl.semaphore_wait(barrier, len(greeted))
    own_everywhere(lambda copy: copy.start())
    for _, d in arrivals:
        acts_out(d).start()
    for load in whole_loads:
        load.wait()
    acts_all[me] = wholes[block_at(me)]


    def relay(zz, sign, c):
        who = zz * LANES + x
        arrived(cot_piece(who, c), c_recv.at[who, c])
        nxt = z + sign
        pl.when(jnp.logical_and(nxt >= 0, nxt < depth))(lambda: z_out(zz, sign, c).start())
        x_out(zz, c).start()

    def relays(k):
        for c in range(CHUNKS):
            pl.when(z - k >= 0)(lambda c=c: relay(z - k, 1, c))
            pl.when(z + k < depth)(lambda c=c: relay(z + k, -1, c))

    def add_term(s, cot, first=False):
        term = lax.dot_general(acts_all[s], cot, (((0,), (0,)), ((), ())),
                               preferred_element_type=jnp.float32)
        total[...] = term if first else total[...] + term

    across = beside + 1 - 2 * (beside % 2)
    sibling_rows = pl.ds(pl.multiple_of(sibling * part, part), part)
    across_rows = pl.ds(pl.multiple_of(across * part, part), part)

    def acts_ready(s):
        arrived(acts_all.at[s, sibling_rows], sib_recv.at[s])
        arrived(acts_all.at[s, across_rows], fwd_recv.at[s])

    add_term(me, cot_ref[...], True)
    for i in range(len(arrivals) + 2):
        if i % LANES == 0 and i // LANES + 1 < depth:
            relays(i // LANES + 1)
        if i < len(arrivals):
            s = arrivals[i][1]
            arrived(acts_all.at[s, my_rows], a_recv.at[s])
            side_out(s, 0).start()
            side_out(s, 1).start()
        if 1 <= i <= len(arrivals):
            s = arrivals[i - 1][1]
            arrived(acts_all.at[s, beside_rows], y_recv.at[s])
            side_out(s, 2).start()
    for is_beside, s in arrivals:
        if not is_beside:
            acts_ready(s)
            add_term(s, cot_all[s])
    for is_beside, s in arrivals:
        if is_beside:
            acts_ready(s)
            for c in range(CHUNKS):
                arrived(cot_piece(s, c), c_recv.at[s, c])
            add_term(s, cot_all[s])
    grad_ref[...] = total[...].astype(grad_ref.dtype)

    own_everywhere(lambda copy: copy.wait_send())
    for d in ordered:
        acts_out(d).wait_send()
    for s in senders:
        for which in range(3):
            side_out(s, which).wait_send()

    def relay_sent(zz, sign, c):
        nxt = z + sign
        pl.when(jnp.logical_and(nxt >= 0, nxt < depth))(lambda: z_out(zz, sign, c).wait_send())
        x_out(zz, c).wait_send()

    for k in range(1, depth):
        for c in range(CHUNKS):
            pl.when(z - k >= 0)(lambda c=c, k=k: relay_sent(z - k, 1, c))
            pl.when(z + k < depth)(lambda c=c, k=k: relay_sent(z + k, -1, c))


def gather_gradient(owner_slot, acts, cotangent, dp_count, mp_count):
    tokens, blk = cotangent.shape
    dma = pltpu.SemaphoreType.DMA
    depth = dp_count // LANES
    vmem = pl.BlockSpec(memory_space=pltpu.VMEM)
    return pl.pallas_call(
        gather_kernel,
        name="gather_gradient",
        out_shape=jax.ShapeDtypeStruct((blk, blk), jnp.bfloat16),
        in_specs=[pl.BlockSpec(memory_space=pltpu.SMEM), pl.BlockSpec(memory_space=pl.ANY), vmem],
        out_specs=vmem,
        scratch_shapes=[
            pltpu.VMEM((dp_count, tokens // mp_count, blk), jnp.bfloat16),
            pltpu.VMEM((dp_count, tokens, blk), jnp.bfloat16),
            pltpu.VMEM((dp_count, tokens, blk), jnp.bfloat16),
            pltpu.VMEM((blk, blk), jnp.float32),
        ] + [dma((dp_count,))] * 8 + [dma((3, CHUNKS)), dma((depth, CHUNKS)), dma((depth, CHUNKS)),
                                     dma((dp_count, CHUNKS)), dma((2, dp_count)),
                                     pltpu.VMEM((dp_count, tokens // mp_count, blk), jnp.bfloat16),
                                     pltpu.VMEM((dp_count, tokens, blk), jnp.bfloat16)],
        compiler_params=pltpu.CompilerParams(collective_id=0, has_side_effects=True),
    )(owner_slot, acts, cotangent)


def mm(former, latter):
    return jnp.dot(former, latter, preferred_element_type=jnp.float32)


def root_kernel(grad_ref, stat_ref, dir_ref, new_ref):
    low = jnp.bfloat16
    blk = grad_ref.shape[0]
    grad = grad_ref[...]
    row = lax.broadcasted_iota(jnp.int32, (blk, blk), 0)
    col = lax.broadcasted_iota(jnp.int32, (blk, blk), 1)
    diagonal = row == col
    grams = [
        lax.dot_general(grad, grad, (((1,), (1,)), ((), ())), preferred_element_type=jnp.float32),
        lax.dot_general(grad, grad, (((0,), (0,)), ((), ())), preferred_element_type=jnp.float32),
    ]
    moments, results, scales = [], [None, None], []
    for side in range(2):
        fresh = BETA * stat_ref[side] + (1.0 - BETA) * grams[side]
        new_ref[side] = fresh
        damped = fresh + jnp.where(diagonal, DAMPING, 0.0)
        frob = jnp.sqrt(jnp.sum(damped * damped, axis=(0, 1), keepdims=True) + EPSILON)
        scales.append(lax.rsqrt(jnp.sqrt(frob)))
        moments.append(damped * (1.0 / frob))
    for iteration in range(ITERS):
        factors = [(jnp.where(diagonal, 5.0, 0.0) - moments[side]) * 0.25 for side in range(2)]
        lows = [factors[side].astype(low) for side in range(2)]
        if iteration + 1 < ITERS:
            squares = [mm(lows[side], lows[side]).astype(low) for side in range(2)]
            inner = [mm(squares[side], moments[side].astype(low)).astype(low) for side in range(2)]
            moments = [mm(squares[side], inner[side]) for side in range(2)]
        for side in range(2):
            results[side] = factors[side] if iteration == 0 else mm(results[side].astype(low), lows[side])
    roots = [(results[side] * scales[side]).astype(low) for side in range(2)]
    direction = mm(mm(roots[0], grad).astype(low), roots[1])
    wide = grad.astype(jnp.float32)
    count = blk * blk
    power = jnp.sum(wide * wide, axis=(0, 1), keepdims=True) / count + EPSILON
    reached = jnp.sum(direction * direction, axis=(0, 1), keepdims=True) / count + EPSILON
    dir_ref[...] = (direction * jnp.sqrt(power / reached)).astype(low)


def apply_roots(grad, stat_pair):
    vmem = pl.BlockSpec(memory_space=pltpu.VMEM)
    return pl.pallas_call(
        root_kernel,
        name="apply_roots",
        out_shape=(jax.ShapeDtypeStruct(grad.shape, jnp.bfloat16),
                   jax.ShapeDtypeStruct(stat_pair.shape, jnp.float32)),
        in_specs=[vmem, vmem],
        out_specs=(vmem, vmem),
    )(grad, stat_pair)


def return_kernel(owner_ref, dir_ref, out_ref, held, send, recv):
    dp_count, piece, blk = held.shape
    me = lax.axis_index("dp")
    others = [(me + step) % dp_count for step in range(1, dp_count)]
    barrier = pltpu.get_barrier_semaphore()
    for d in others:
        pl.semaphore_signal(barrier, inc=1, device_id={"dp": d}, device_id_type=MESH)
    pl.semaphore_wait(barrier, len(others))

    def rows_of(d):
        return pl.ds(pl.multiple_of(d * piece, piece), piece)

    far_first = sorted(range(1, dp_count), key=lambda step: -min(step, dp_count - step))
    copies = []
    for step in far_first:
        d = (me + step) % dp_count
        copy = pltpu.make_async_remote_copy(
            src_ref=dir_ref.at[rows_of(d)], dst_ref=held.at[me], send_sem=send.at[d],
            recv_sem=recv.at[me], device_id={"dp": d}, device_id_type=MESH)
        copy.start()
        copies.append(copy)
    held[me] = dir_ref[rows_of(me)]
    for d in others:
        pltpu.make_async_copy(held.at[d], held.at[d], recv.at[d]).wait()
    for w in range(dp_count):
        out_ref[w] = held[owner_ref[w]]
    for copy in copies:
        copy.wait_send()


def return_rows(owner_slot, direction, dp_count):
    blk = direction.shape[0]
    shape = (dp_count, blk // dp_count, blk)
    vmem = pl.BlockSpec(memory_space=pltpu.VMEM)
    dma = pltpu.SemaphoreType.DMA
    return pl.pallas_call(
        return_kernel,
        name="return_rows",
        out_shape=jax.ShapeDtypeStruct(shape, jnp.bfloat16),
        in_specs=[pl.BlockSpec(memory_space=pltpu.SMEM), vmem],
        out_specs=vmem,
        scratch_shapes=[pltpu.VMEM(shape, jnp.bfloat16), dma((dp_count,)), dma((dp_count,))],
        compiler_params=pltpu.CompilerParams(collective_id=1, has_side_effects=True),
    )(owner_slot, direction)


def full_house(acts, cotangent, stats, owner_slot):
    dp_count, mp_count = lax.axis_size("dp"), lax.axis_size("mp")
    grad = gather_gradient(owner_slot, acts, cotangent, dp_count, mp_count)
    direction, new_pair = apply_roots(grad, stats[0, 0])
    return return_rows(owner_slot, direction, dp_count), new_pair[None, None]


def device_body(acts, cotangent, stats, owner_slot):
    dp_count, mp_count = lax.axis_size("dp"), lax.axis_size("mp")
    blk = cotangent.shape[1]
    every_slot_filled = stats.shape[1] == 1 and acts.shape[1] == dp_count * blk
    if every_slot_filled and mp_count == 4 and dp_count % LANES == 0 and dp_count <= 8:
        return full_house(acts, cotangent, stats, owner_slot)
    return on_device(acts, cotangent, stats, owner_slot)


def solution(mesh):
    return jax.shard_map(
        device_body,
        mesh=mesh,
        in_specs=(P("dp", None), P("dp", "mp"), P("mp", "dp", None, None, None), P()),
        out_specs=(P(None, "dp", "mp"), P("mp", "dp", None, None, None)),
        check_vma=False,
    )
```
